32 devices in a mesh: row: 8 (over y, x, core), col: 4 (over z).
Axes of the slice: x: 2, y: 2, z: 4, core: 2. Of those that a mesh axis runs over, the one named last changes fastest.
Arguments:
- a_matrix: float32 [2048, 2048], P('row', 'col'), may hold values from -0.9 to 0.9
- b_matrix: float32 [2048, 2048], P('row', 'col'), may hold values from -0.9 to 0.9
- a_panel: float32 [2048, 1024], P('row', 'col'), may hold values from -0.9 to 0.9
- b_panel: float32 [2048, 1024], P('row', 'col'), may hold values from -0.9 to 0.9
Outputs:
- triangle: float32 [1024, 1024], P('row', 'col')
- pencil_cross: float32 [2048, 2048], P('row', 'col')
The draws below stay inside these ranges and needn't reach their ends.
All inputs are finite; a program needn't handle non-finite values.
Results may differ from the reference program's by a relative error of at most 0.0003.
Values sent between devices are 32-bit elements; how exact they have to be, the bound alone decides.
No kernel may reach another device: no remote copies, remote signals or barrier semaphores. Data moves between devices by JAX's collectives and lax.ppermute only.
A program may use at most 64 MiB of HBM per device.

```python
import jax
import jax.numpy as jnp
from jax import lax

N = 2048
K = 1024


def block_scale(rng, dims, cuts, low, high):
    loudness = 1.0
    for position, parts in cuts:
        heights = jax.random.uniform(jax.random.fold_in(jax.random.fold_in(rng, 6), position), (parts,), jnp.float32, low / len(cuts), high / len(cuts))
        loudness = loudness * jnp.repeat(jnp.exp(heights), dims[position] // parts).reshape((-1,) + (1,) * (len(dims) - 1 - position))
    return loudness


def scatter_about(key, shape, deviation, most, cuts=(), held_as=jnp.bfloat16):
    array = deviation * jax.random.normal(key, shape, jnp.float32)
    if cuts:
        array = array * block_scale(key, shape, cuts, -0.22, 0.18)
    return jnp.clip(array, -most, most).astype(held_as)


def setup_inputs(seed: int = 0) -> dict:
    splits = jax.random.split(jax.random.key(seed), 5)
    a_matrix = scatter_about(splits[0], (N, N), 0.15, 0.9, ((0, 8), (1, 4)), jnp.float32)
    b_matrix = scatter_about(splits[1], (N, N), 0.15, 0.9, ((0, 8), (1, 4)), jnp.float32)
    a_panel = scatter_about(splits[2], (N, K), 0.15, 0.9, ((0, 8), (1, 4)), jnp.float32)
    b_panel = scatter_about(splits[3], (N, K), 0.15, 0.9, ((0, 8), (1, 4)), jnp.float32)
    return {"a_matrix": a_matrix, "b_matrix": b_matrix, "a_panel": a_panel, "b_panel": b_panel}


HIGHEST = lax.Precision.HIGHEST

def reference(a_matrix, b_matrix, a_panel, b_panel):
    stacked = jnp.concatenate([b_panel, -a_panel], 0)
    q_full, r_full = jnp.linalg.qr(stacked)
    diag_signs = jnp.sign(jnp.diagonal(r_full))
    triangle = r_full * diag_signs[:, None]
    q_full = q_full * diag_signs[None, :]
    upper_rows = q_full[:N]
    lower_rows = q_full[N:]
    z_block = jnp.dot(lower_rows.T, b_matrix, precision=HIGHEST)
    v_block = jnp.dot(upper_rows, z_block, precision=HIGHEST)
    pencil_cross = -jnp.dot(a_matrix.T, v_block, precision=HIGHEST)
    return (triangle, pencil_cross)
```

```python
import jax
import jax.numpy as jnp
from jax import lax
from jax.experimental import pallas as pl
from jax.experimental.pallas import tpu as pltpu
from jax.sharding import PartitionSpec as P

F32 = jnp.float32
BF16 = jnp.bfloat16
HIGHEST = lax.Precision.HIGHEST
NB = 128
SB = 16


def split3(x):
    hi=x.astype(BF16); r=x-hi.astype(F32)
    mid=r.astype(BF16); lo=(r-mid.astype(F32)).astype(BF16)
    return hi,mid,lo
def split2(x):
    hi=x.astype(BF16); lo=(x-hi.astype(F32)).astype(BF16)
    return hi,lo

def factor_block(diag):
    rows=lax.broadcasted_iota(jnp.int32,(NB,NB),0); cols=lax.broadcasted_iota(jnp.int32,(NB,NB),1)
    work=jnp.concatenate([diag,jnp.where(rows==cols,1.0,0.0).astype(F32)],1)
    sub=lax.broadcasted_iota(jnp.int32,(SB,NB),0)
    done=[]
    for s in range(NB//SB):
        j0=s*SB
        block=work[:SB]
        col=[jnp.broadcast_to(block[:,j0+t:j0+t+1],(SB,NB)) for t in range(SB)]
        left,right=block[:,:NB],block[:,NB:]
        scale=jnp.zeros((SB,NB),F32)
        for t in range(SB):
            ct=col[t]
            inv_root=lax.rsqrt(jnp.broadcast_to(ct[t:t+1],(SB,NB)))
            scale=jnp.where(sub==t,inv_root,scale)
            if t==SB-1: break
            mult=jnp.where(sub>t,ct,0.0)*(inv_root*inv_root)
            for u in range(t+1,SB):
                col[u]=col[u]-mult*jnp.broadcast_to(ct[u:u+1],(SB,NB))
            left=left-mult*jnp.broadcast_to(left[t:t+1],(SB,NB))
            right=right-mult*jnp.broadcast_to(right[t:t+1],(SB,NB))
        left=left*scale; right=right*scale
        final=jnp.concatenate([left,right],1)
        done.append(final)
        if s<NB//SB-1:
            hi,mid,lo=split3(final)
            lhs=jnp.concatenate([hi,hi,hi,mid,mid,lo],0)[:,:NB]
            rhs=jnp.concatenate([hi,mid,lo,hi,mid,hi],0)
            upd=lax.dot_general(lhs,rhs,(((0,),(0,)),((),())),preferred_element_type=F32)
            work=work[SB:]-upd[j0+SB:]
    full=jnp.concatenate(done,0)
    return jnp.where(rows<=cols,full[:,:NB],0.0),full[:,NB:]

def chol_kernel(g_ref,r_ref,w_ref):
    k_total=g_ref.shape[0]//NB
    n=g_ref.shape[0]
    for i in range(k_total):
        r_ref[i*NB:(i+1)*NB,i*NB:]=g_ref[i*NB:(i+1)*NB,i*NB:]
        if i: r_ref[i*NB:(i+1)*NB,:i*NB]=jnp.zeros((NB,i*NB),F32)
    for k in range(k_total):
        a,b=k*NB,(k+1)*NB
        fac,inv=factor_block(r_ref[a:b,a:b])
        r_ref[a:b,a:b]=fac
        w_ref[a:b,:]=inv
        if b==n: break
        panel=jnp.dot(inv,r_ref[a:b,b:],precision=HIGHEST,preferred_element_type=F32)
        r_ref[a:b,b:]=panel
        for i in range(k+1,k_total):
            c,d=i*NB,(i+1)*NB
            lhs=panel[:,c-b:d-b]; rhs=panel[:,c-b:]
            r_ref[c:d,c:]=r_ref[c:d,c:]-lax.dot_general(lhs,rhs,(((0,),(0,)),((),())),precision=HIGHEST,preferred_element_type=F32)

def chol(g):
    n=g.shape[0]
    return pl.pallas_call(chol_kernel,out_shape=(jax.ShapeDtypeStruct((n,n),F32),jax.ShapeDtypeStruct((n,NB),F32)),
        name="chol",compiler_params=pltpu.CompilerParams(vmem_limit_bytes=48*2**20))(g)

def solve_kernel(x_ref,r_ref,w_ref,o_ref,v_ref):
    n=r_ref.shape[0]; m=o_ref.shape[0]
    v_ref[...]=x_ref[...]
    NT=(((1,),(1,)),((),()))
    for k in range(n//NB):
        a,b=k*NB,(k+1)*NB
        xh,xl=split2(v_ref[:,a:b]); wh,wl=split2(w_ref[a:b,:])
        vk=lax.dot_general(jnp.concatenate([xh,xh,xl],1),jnp.concatenate([wh,wl,wh],1),NT,preferred_element_type=F32)
        v_ref[:,a:b]=vk
        if b<n:
            vh,vl=split2(vk); rh,rl=split2(r_ref[a:b,b:])
            v_ref[:,b:]=v_ref[:,b:]-jnp.dot(jnp.concatenate([vh,vh,vl],1),jnp.concatenate([rh,rl,rh],0),preferred_element_type=F32)
    vh,vl=split2(v_ref[...])
    o_ref[...]=lax.dot_general(jnp.concatenate([vh[:m],vh[:m],vl[:m]],1),jnp.concatenate([vh[m:],vl[m:],vh[m:]],1),NT,preferred_element_type=F32)

def solve(x,r,w,m):
    return pl.pallas_call(solve_kernel,out_shape=jax.ShapeDtypeStruct((m,x.shape[0]-m),F32),
        scratch_shapes=[pltpu.VMEM(x.shape,F32)],name="solve",
        compiler_params=pltpu.CompilerParams(vmem_limit_bytes=48*2**20))(x,r,w)


TN = (((0,), (0,)), ((), ()))


def local(a_matrix, b_matrix, a_panel, b_panel):
    row_axis, col_axis = lax.axis_size("row"), lax.axis_size("col")
    row_index, col_index = lax.axis_index("row"), lax.axis_index("col")
    rows, width = a_panel.shape
    own = jnp.concatenate([b_panel, a_panel], 0)
    full = lax.all_gather(own, "col", axis=1, tiled=True)
    full_b, full_a = full[:rows], full[rows:]
    order = width * col_axis
    part = lax.dot_general(own, full, TN, precision=HIGHEST)
    share = width // row_axis
    pieces = lax.all_to_all(part.reshape(row_axis, share, order), "row", 0, 0, tiled=True)
    gram_piece = jnp.sum(pieces, 0)
    gram_cols = lax.all_gather(gram_piece, "col", axis=0, tiled=False)
    gram = lax.all_gather(gram_cols, "row", axis=1, tiled=False).reshape(order, order)
    part_x = lax.dot_general(a_matrix, full_b, TN, precision=HIGHEST)
    part_y = lax.dot_general(b_matrix, full_a, TN, precision=HIGHEST)
    x_piece = lax.psum_scatter(part_x, "row", scatter_dimension=0, tiled=True)
    y_rows = lax.psum(part_y, "row")
    ratio = row_axis // col_axis
    moves = [
        (r * col_axis + c, (c * ratio + r // col_axis) * col_axis + r % col_axis)
        for r in range(row_axis)
        for c in range(col_axis)
    ]
    x_piece = lax.ppermute(x_piece, ("row", "col"), moves)
    x_rows = lax.all_gather(x_piece, "col", axis=0, tiled=True)
    upper, inverses = chol(gram)
    both = jnp.concatenate([x_rows, y_rows], 0)
    pencil_cross = solve(both, upper, inverses, x_rows.shape[0])
    tri_rows = order // row_axis
    triangle = lax.dynamic_slice(upper, (row_index * tri_rows, col_index * width), (tri_rows, width))
    return triangle, pencil_cross


def solution(mesh):
    specs = (P("row", "col"),) * 4
    return jax.shard_map(local, mesh=mesh, in_specs=specs, out_specs=(P("row", "col"),) * 2, check_vma=False)
```
